32 devices in a mesh: expert: 16 (over z, y, x), tensor: 2 (over core).
Axes of the slice: x: 2, y: 2, z: 4, core: 2. Of those that a mesh axis runs over, the one named last changes fastest.
Arguments:
- states: bfloat16 [2048, 1536], P('expert'), may hold values from -60 to 60
- norm_gain: float32 [1536], replicated, may hold values from 0.25 to 1.75
- router: bfloat16 [1536, 8], replicated, may hold values from -0.15625 to 0.15625
- w_gate: bfloat16 [16, 1536, 2048], P('expert', None, 'tensor'), may hold values from -0.15625 to 0.15625
- w_up: bfloat16 [16, 1536, 2048], P('expert', None, 'tensor'), may hold values from -0.15625 to 0.15625
- w_down: bfloat16 [16, 2048, 1536], P('expert', 'tensor'), may hold values from -0.09375 to 0.09375
- expert_ids: int32 [2048, 2], P('expert'), may hold values from 0 to 7, as said below
- slot_pos: int32 [2048, 2], P('expert'), may hold values from 0 to 41, as said below
- keep_mask: int32 [2048, 2], P('expert'), may hold values from 0 to 1, as said below
Outputs:
- next_states: bfloat16 [2048, 1536], P('expert')
The draws below stay inside these ranges and needn't reach their ends.
Inputs may be any that keep to these rules, and one draw needn't show every extreme that they name: `expert_ids`: each row names two different experts; in every block of 128 rows one expert is named by more than 41 rows. `slot_pos`: for each choice, the number of earlier choices of the same expert within the same block of 128 rows, counted row by row with a row's first choice before its second, or 41 where that number is 41 or more. `keep_mask`: 1 exactly where slot_pos is under 41; in every block of 128 rows some expert has all 41 slots filled.
All inputs are finite; a program needn't handle non-finite values.
Results may differ from the reference program's by a relative error of at most 0.0038.
Values may be sent and summed in bfloat16 or wider, within the bound.
A program may use at most 64 MiB of HBM per device.

```python
import math
import jax
import jax.numpy as jnp
from jax import lax

D = 1536
FF = 4096
TOP = 2
SHARE = 2
TOK_DEV = 128
EXPERTS = 8
TOKENS = 2048
CAP = 41


def draw_states(key, part):
    keys = jax.random.split(jax.random.fold_in(key, 11), 3)
    row_scale = jnp.exp(jax.random.uniform(keys[0], (TOKENS, 1), minval=math.log(0.3), maxval=math.log(3.0)))
    col_scale = jnp.exp(jax.random.uniform(keys[1], (1, D), minval=math.log(0.4), maxval=math.log(4.0)))
    base = jnp.clip(jax.random.normal(keys[2], (TOKENS, D)), -4.0, 4.0)
    return (base * row_scale * col_scale).astype(jnp.bfloat16)


def routing_tables(key):
    keys = jax.random.split(jax.random.fold_in(key, 7), 5)
    order = jax.random.permutation(keys[0], EXPERTS)
    first_draw = jax.random.randint(keys[1], (TOKENS,), 0, EXPERTS)
    second_draw = jax.random.randint(keys[2], (TOKENS,), 0, EXPERTS)
    first_choice = order[jnp.minimum(first_draw, second_draw)]
    hot_expert = jax.random.randint(keys[3], (), 0, EXPERTS)
    row_in_block = jnp.arange(TOKENS) % TOK_DEV
    first_choice = jnp.where(row_in_block <= CAP, hot_expert, first_choice)
    offsets = jax.random.randint(keys[4], (TOKENS,), 1, EXPERTS)
    second_choice = (first_choice + offsets) % EXPERTS
    chosen_ids = jnp.stack([first_choice, second_choice], axis=1).astype(jnp.int32)
    flat_ids = chosen_ids.reshape(TOKENS // TOK_DEV, TOK_DEV * TOP)
    one_hot = (flat_ids[:, :, None] == jnp.arange(EXPERTS)[None, None, :]).astype(jnp.int32)
    earlier = jnp.cumsum(one_hot, axis=1) - one_hot
    positions = jnp.sum(earlier * one_hot, axis=-1).reshape(TOKENS, TOP).astype(jnp.int32)
    kept_flags = (positions < CAP).astype(jnp.int32)
    positions = jnp.minimum(positions, CAP).astype(jnp.int32)
    return (chosen_ids, positions, kept_flags)


def draw_expert_ids(key, part):
    return routing_tables(key)[0]


def draw_slot_pos(key, part):
    return routing_tables(key)[1]


def draw_keep_mask(key, part):
    return routing_tables(key)[2]


def shard_levels(rng, shape, pieces, least, largest):
    level, own = 1.0, jax.random.fold_in(rng, 6)
    for axis_at, parts in pieces:
        steps = jnp.exp(jax.random.uniform(jax.random.fold_in(own, axis_at), (parts,), jnp.float32, least / len(pieces), largest / len(pieces)))
        level = level * jnp.repeat(steps, shape[axis_at] // parts).reshape([-1 if axis == axis_at else 1 for axis in range(len(shape))])
    return level


def normal_values(stream_key, dims, spread, bound, pieces=(), dtype=jnp.bfloat16):
    array = spread * jax.random.normal(stream_key, dims, jnp.float32)
    if pieces:
        array = array * shard_levels(stream_key, dims, pieces, -0.22, 0.18)
    return jnp.clip(array, -bound, bound).astype(dtype)


def setup_inputs(seed: int = 0) -> dict:
    arg_keys = jax.random.split(jax.random.key(seed), 10)
    return {
        "states": draw_states(jax.random.fold_in(arg_keys[9], 71), 0),
        "norm_gain": jnp.clip(1.0 + 0.15 * jax.random.normal(arg_keys[1], (D,), jnp.float32), 0.25, 1.75),
        "router": normal_values(arg_keys[2], (D, EXPERTS), D ** -0.5, 0.15625),
        "w_gate": normal_values(arg_keys[3], (EXPERTS * SHARE, D, FF // SHARE), D ** -0.5, 0.15625, ((0, 16), (2, 2))),
        "w_up": normal_values(arg_keys[4], (EXPERTS * SHARE, D, FF // SHARE), D ** -0.5, 0.15625, ((0, 16), (2, 2))),
        "w_down": normal_values(arg_keys[5], (EXPERTS * SHARE, FF // SHARE, D), FF ** -0.5, 0.09375, ((0, 16), (1, 2))),
        "expert_ids": draw_expert_ids(jax.random.fold_in(arg_keys[9], 71), 0),
        "slot_pos": draw_slot_pos(jax.random.fold_in(arg_keys[9], 71), 0),
        "keep_mask": draw_keep_mask(jax.random.fold_in(arg_keys[9], 71), 0),
    }


def expert_ffn(operands):
    slot_rows, gate_parts, up_parts, down_parts = operands
    gate_mat = jnp.concatenate([gate_parts[h] for h in range(SHARE)], axis=1)
    up_mat = jnp.concatenate([up_parts[h] for h in range(SHARE)], axis=1)
    down_mat = down_parts.reshape(FF, D)
    flat_rows = slot_rows.reshape(-1, D)
    gate_act = jnp.dot(flat_rows, gate_mat, preferred_element_type=jnp.float32)
    up_act = jnp.dot(flat_rows, up_mat, preferred_element_type=jnp.float32)
    hidden = (jax.nn.silu(gate_act) * up_act).astype(jnp.bfloat16)
    result = jnp.dot(hidden, down_mat, preferred_element_type=jnp.float32).astype(jnp.bfloat16)
    return result.reshape(slot_rows.shape)

def reference(states, norm_gain, router, w_gate, w_up, w_down, expert_ids, slot_pos, keep_mask):
    values = states.astype(jnp.float32)
    normed = (values * lax.rsqrt(lax.optimization_barrier(jnp.mean(values * values, axis=-1, keepdims=True)) + 1e-06) * norm_gain).astype(jnp.bfloat16)
    logits = jnp.dot(normed, router, preferred_element_type=jnp.float32)
    chosen = jnp.take_along_axis(logits, expert_ids, axis=1)
    gate_score = jax.nn.sigmoid(chosen)
    weight = gate_score / lax.optimization_barrier(jnp.sum(gate_score, axis=1, keepdims=True))
    num_blocks = TOKENS // TOK_DEV
    block_id = (jnp.arange(TOKENS) // TOK_DEV).astype(jnp.int32)
    is_kept = keep_mask > 0
    target_expert = jnp.where(is_kept, expert_ids, EXPERTS).astype(jnp.int32)
    block_index = jnp.broadcast_to(block_id[:, None], expert_ids.shape)
    updates = jnp.broadcast_to(normed[:, None, :], (TOKENS, TOP, D))
    slot_buffer = jnp.zeros((EXPERTS, num_blocks, CAP, D), jnp.bfloat16)
    slot_buffer = slot_buffer.at[target_expert, block_index, slot_pos].set(updates, mode='drop')
    gate_split = w_gate.reshape(EXPERTS, SHARE, D, FF // SHARE)
    up_split = w_up.reshape(EXPERTS, SHARE, D, FF // SHARE)
    down_split = w_down.reshape(EXPERTS, SHARE, FF // SHARE, D)
    expert_out = lax.map(expert_ffn, (slot_buffer, gate_split, up_split, down_split))
    safe_pos = jnp.minimum(slot_pos, CAP - 1).astype(jnp.int32)
    picked = expert_out[expert_ids, block_index, safe_pos].astype(jnp.float32)
    factor = jnp.where(is_kept, weight, 0.0).astype(jnp.float32)
    combined = lax.optimization_barrier(jnp.sum(factor[:, :, None] * picked, axis=1))
    return (values + combined).astype(jnp.bfloat16)
```

```python
import functools

import jax
import jax.numpy as jnp
from jax import lax
from jax.experimental import pallas as pl
from jax.experimental.pallas import tpu as pltpu
from jax.sharding import PartitionSpec as P

MESH = pl.DeviceIdType.MESH


def flip(value, mask):
    result = value
    bit = 1
    while bit <= mask:
        if mask & bit:
            result = result + bit * (1 - 2 * (value // bit % 2))
        bit *= 2
    return result


def peer_order(count):
    rest = list(range(1, count))
    return [0] + sorted(rest, key=lambda i: (bin(i).count("1"), -i))


def kernel(
    experts, capacity, padded,
    states_ref, gain_ref, router_ref, ids_ref, pos_ref, keep_ref, wg_hbm, wu_hbm, wd_hbm,
    out_ref,
    wg, wu, wd, sent, rows, hid, give, got, acc, cross, crossed, result, back, final,
    w_sem, a_send, a_recv, c_send, c_recv, x_send, x_recv,
    p_send, p_recv, r_send, r_recv, o_send, o_recv, f_send, f_recv,
):
    idx = lax.axis_index("expert")
    core = lax.axis_index("tensor")
    group, side = idx // 2, idx % 2
    other_side, other_core = 1 - side, 1 - core
    tok, width = states_ref.shape
    half = width // 2
    slots = experts * padded
    order = peer_order(experts)
    tile = 256
    neighbour = (group * 2 + other_side, core)
    sibling = (idx, other_core)

    loads = [
        pltpu.make_async_copy(src.at[0], dst, w_sem.at[n])
        for n, (src, dst) in enumerate(((wg_hbm, wg), (wu_hbm, wu), (wd_hbm, wd)))
    ]
    for load in loads:
        load.start()

    barrier = pltpu.get_barrier_semaphore()
    peers = [(flip(group, i) * 2 + side, core) for i in order]
    for peer in peers[1:] + [neighbour, sibling]:
        pl.semaphore_signal(barrier, inc=1, device_id=peer, device_id_type=MESH)

    values = states_ref[...].astype(jnp.float32)
    scale = lax.rsqrt(jnp.mean(values * values, axis=-1, keepdims=True) + 1e-06)
    normed = (values * scale * gain_ref[...]).astype(jnp.bfloat16)
    ids = ids_ref[...]
    kept = keep_ref[...] > 0
    place = jnp.where(kept, ids * padded + pos_ref[...], -1)
    column = lax.broadcasted_iota(jnp.int32, (tok, slots), 1)
    first = column == place[:, 0:1]
    second = column == place[:, 1:2]
    table = jnp.where(first | second, 1.0, 0.0).astype(jnp.bfloat16)
    mine = jnp.where(core == 0, normed[:, :half], normed[:, half:])
    sent[...] = (
        lax.dot_general(table, mine, (((0,), (0,)), ((), ())), preferred_element_type=jnp.float32)
        .astype(jnp.bfloat16)
        .reshape(experts, padded, half)
    )
    pl.semaphore_wait(barrier, experts + 1)

    pending = []

    def remote(src, dst, send, recv, peer):
        return pltpu.make_async_remote_copy(
            src_ref=src, dst_ref=dst, send_sem=send, recv_sem=recv,
            device_id=peer, device_id_type=MESH,
        )

    def launch(copy):
        copy.start()
        pending.append(copy)

    own = pltpu.make_async_copy(sent.at[group], rows.at[core, side, group], a_recv.at[group])
    own.start()
    for i, peer in zip(order[1:], peers[1:]):
        launch(remote(
            sent.at[flip(group, i)], rows.at[core, side, group],
            a_send.at[flip(group, i)], a_recv.at[group], peer,
        ))

    logits = jnp.dot(normed, router_ref[...], preferred_element_type=jnp.float32)
    expert_column = lax.broadcasted_iota(jnp.int32, (tok, experts), 1)
    score = [
        jax.nn.sigmoid(
            jnp.sum(jnp.where(expert_column == ids[:, n : n + 1], logits, 0.0), axis=1, keepdims=True)
        )
        for n in range(2)
    ]
    total = score[0] + score[1]
    mix = jnp.where(first, score[0] / total, 0.0) + jnp.where(second, score[1] / total, 0.0)
    mix_high = mix.astype(jnp.bfloat16)
    mix_low = (mix - mix_high.astype(jnp.float32)).astype(jnp.bfloat16)

    def share(which, g):
        launch(remote(
            rows.at[core, which, g], rows.at[core, which, g],
            c_send.at[which, g], c_recv.at[which, g], sibling,
        ))

    def take_neighbour(g):
        remote(
            rows.at[core, other_side, g], rows.at[core, other_side, g],
            x_send.at[g], x_recv.at[g], neighbour,
        ).wait_recv()
        share(other_side, g)

    lag = 2
    for n, i in enumerate(order):
        g = flip(group, i)
        if i == 0:
            own.wait()
        else:
            remote(
                sent.at[g], rows.at[core, side, g], a_send.at[g], a_recv.at[g], peers[n]
            ).wait_recv()
        launch(remote(
            rows.at[core, side, g], rows.at[core, side, g], x_send.at[g], x_recv.at[g], neighbour
        ))
        share(side, g)
        if n >= lag:
            take_neighbour(flip(group, order[n - lag]))
    for n in range(max(0, experts - lag), experts):
        take_neighbour(flip(group, order[n]))

    for load in loads:
        load.wait()

    def feed_forward(which):
        for i in order:
            g = flip(group, i)
            remote(
                rows.at[other_core, which, g], rows.at[other_core, which, g],
                c_send.at[which, g], c_recv.at[which, g], sibling,
            ).wait_recv()

        @pl.loop(0, hid.shape[1] // tile)
        def _(n):
            cols = pl.ds(pl.multiple_of(n * tile, tile), tile)
            low = rows[0, which].reshape(slots, half)
            high = rows[1, which].reshape(slots, half)

            def project(w):
                return jnp.dot(
                    low, w[:half, cols], preferred_element_type=jnp.float32
                ) + jnp.dot(high, w[half:, cols], preferred_element_type=jnp.float32)

            hid[:, cols] = (jax.nn.silu(project(wg)) * project(wu)).astype(jnp.bfloat16)

        def down(which_half, n):
            cols = pl.ds(pl.multiple_of(which_half * half + n * tile, tile), tile)
            return jnp.dot(hid[...], wd[:, cols], preferred_element_type=jnp.float32)

        @pl.loop(0, half // tile)
        def _(n):
            cols = pl.ds(pl.multiple_of(n * tile, tile), tile)
            give[which, :, cols] = down(other_core, n).astype(jnp.bfloat16)

        launch(remote(give.at[which], got.at[which], p_send.at[which], p_recv.at[which], sibling))

        @pl.loop(0, half // tile)
        def _(n):
            cols = pl.ds(pl.multiple_of(n * tile, tile), tile)
            acc[which, :, cols] = down(core, n)

    def chip_sum(which, g):
        at = pl.ds(pl.multiple_of(g * padded, padded), padded)
        return acc[which, at, :] + got[which, at, :].astype(jnp.float32)

    def wait_sibling(which):
        remote(
            give.at[which], got.at[which], p_send.at[which], p_recv.at[which], sibling
        ).wait_recv()

    feed_forward(other_side)
    wait_sibling(other_side)
    for i in order:
        g = flip(group, i)
        cross[g] = chip_sum(other_side, g).astype(jnp.bfloat16)
        launch(remote(cross.at[g], crossed.at[g], r_send.at[g], r_recv.at[g], neighbour))

    feed_forward(side)
    wait_sibling(side)
    for n, i in enumerate(order):
        g = flip(group, i)
        remote(cross.at[g], crossed.at[g], r_send.at[g], r_recv.at[g], neighbour).wait_recv()
        whole = (chip_sum(side, g) + crossed[g].astype(jnp.float32)).astype(jnp.bfloat16)
        if i == 0:
            back[g] = whole
        else:
            result[g] = whole
            launch(remote(result.at[g], back.at[group], o_send.at[g], o_recv.at[group], peers[n]))

    for n, i in enumerate(order[1:], 1):
        g = flip(group, i)
        remote(result.at[g], back.at[g], o_send.at[g], o_recv.at[g], peers[n]).wait_recv()
    returned = back[...].reshape(slots, half)
    combined = jnp.dot(mix_high, returned, preferred_element_type=jnp.float32) + jnp.dot(
        mix_low, returned, preferred_element_type=jnp.float32
    )
    residual = jnp.where(core == 0, states_ref[:, :half], states_ref[:, half:]).astype(jnp.float32)
    final[core] = (residual + combined).astype(jnp.bfloat16)
    last = remote(final.at[core], final.at[core], f_send, f_recv, sibling)
    last.start()
    remote(final.at[other_core], final.at[other_core], f_send, f_recv, sibling).wait_recv()
    out_ref[:, :half] = final[0]
    out_ref[:, half:] = final[1]
    last.wait_send()
    for copy in pending:
        copy.wait_send()


def per_device(states, norm_gain, router, w_gate, w_up, w_down, expert_ids, slot_pos, keep_mask):
    tok, width = states.shape
    groups = lax.axis_size("expert")
    experts = router.shape[1]
    assert groups == 2 * experts and lax.axis_size("tensor") == 2
    capacity = max(2, 5 * tok // (2 * experts) + 1)
    padded = -(-capacity // 16) * 16
    half = width // 2
    slots = experts * padded
    units = w_gate.shape[2]
    bf16, f32 = jnp.bfloat16, jnp.float32
    dma = pltpu.SemaphoreType.DMA
    vmem = pl.BlockSpec(memory_space=pltpu.VMEM)
    hbm = pl.BlockSpec(memory_space=pl.ANY)
    return pl.pallas_call(
        functools.partial(kernel, experts, capacity, padded),
        out_shape=jax.ShapeDtypeStruct((tok, width), bf16),
        in_specs=[vmem] * 6 + [hbm] * 3,
        out_specs=vmem,
        scratch_shapes=[
            pltpu.VMEM((width, units), bf16),
            pltpu.VMEM((width, units), bf16),
            pltpu.VMEM((units, width), bf16),
            pltpu.VMEM((experts, padded, half), bf16),
            pltpu.VMEM((2, 2, experts, padded, half), bf16),
            pltpu.VMEM((slots, units), bf16),
            pltpu.VMEM((2, slots, half), bf16),
            pltpu.VMEM((2, slots, half), bf16),
            pltpu.VMEM((2, slots, half), f32),
            pltpu.VMEM((experts, padded, half), bf16),
            pltpu.VMEM((experts, padded, half), bf16),
            pltpu.VMEM((experts, padded, half), bf16),
            pltpu.VMEM((experts, padded, half), bf16),
            pltpu.VMEM((2, tok, half), bf16),
            dma((3,)),
            dma((experts,)), dma((experts,)),
            dma((2, experts)), dma((2, experts)),
            dma((experts,)), dma((experts,)),
            dma((2,)), dma((2,)),
            dma((experts,)), dma((experts,)),
            dma((experts,)), dma((experts,)),
            dma, dma,
        ],
        compiler_params=pltpu.CompilerParams(
            collective_id=0, has_side_effects=True, vmem_limit_bytes=60 * 1024 * 1024
        ),
    )(states, norm_gain.reshape(1, width), router, expert_ids, slot_pos, keep_mask, w_gate, w_up, w_down)


def solution(mesh):
    placed = (
        P("expert", None),
        P(),
        P(),
        P("expert", None, "tensor"),
        P("expert", None, "tensor"),
        P("expert", "tensor", None),
        P("expert", None),
        P("expert", None),
        P("expert", None),
    )
    return jax.shard_map(
        per_device, mesh=mesh, in_specs=placed, out_specs=P("expert", None), check_vma=False
    )
```

```python
import functools

import jax
import jax.numpy as jnp
from jax import lax
from jax.experimental import pallas as pl
from jax.experimental.pallas import tpu as pltpu
from jax.sharding import PartitionSpec as P

MESH = pl.DeviceIdType.MESH


def flip(value, mask):
    result = value
    bit = 1
    while bit <= mask:
        if mask & bit:
            result = result + bit * (1 - 2 * (value // bit % 2))
        bit *= 2
    return result


def peer_order(count):
    rest = list(range(1, count))
    return [0] + sorted(rest, key=lambda i: (bin(i).count("1"), -i))


def kernel(
    experts, capacity, padded,
    states_ref, gain_ref, router_ref, ids_ref, pos_ref, keep_ref, wg_hbm, wu_hbm, wd_hbm,
    out_ref,
    wg, wu, wd, sent, rows, hid, give, got, acc, cross, crossed, result, back, final,
    w_sem, a_send, a_recv, c_send, c_recv, x_send, x_recv,
    p_send, p_recv, r_send, r_recv, o_send, o_recv, f_send, f_recv,
):
    idx = lax.axis_index("expert")
    core = lax.axis_index("tensor")
    group, side = idx // 2, idx % 2
    other_side, other_core = 1 - side, 1 - core
    tok, width = states_ref.shape
    half = width // 2
    slots = experts * padded
    order = peer_order(experts)
    tile = 256
    neighbour = (group * 2 + other_side, core)
    sibling = (idx, other_core)

    loads = [
        pltpu.make_async_copy(src.at[0], dst, w_sem.at[n])
        for n, (src, dst) in enumerate(((wg_hbm, wg), (wu_hbm, wu), (wd_hbm, wd)))
    ]
    for load in loads:
        load.start()

    barrier = pltpu.get_barrier_semaphore()
    peers = [(flip(group, i) * 2 + side, core) for i in order]
    for peer in peers[1:] + [neighbour, sibling]:
        pl.semaphore_signal(barrier, inc=1, device_id=peer, device_id_type=MESH)

    values = states_ref[...].astype(jnp.float32)
    scale = lax.rsqrt(jnp.mean(values * values, axis=-1, keepdims=True) + 1e-06)
    normed = (values * scale * gain_ref[...].reshape(1, width)).astype(jnp.bfloat16)
    ids = ids_ref[...]
    kept = keep_ref[...] > 0
    place = jnp.where(kept, ids * padded + pos_ref[...], -1)
    slot = lax.broadcasted_iota(jnp.int32, (slots, tok), 0)
    first = slot == place[0:1, :]
    second = slot == place[1:2, :]
    table = jnp.where(first | second, 1.0, 0.0).astype(jnp.bfloat16)
    mine = jnp.where(core == 0, normed[:, :half], normed[:, half:])
    sent[...] = (
        jnp.dot(table, mine, preferred_element_type=jnp.float32)
        .astype(jnp.bfloat16)
        .reshape(experts, padded, half)
    )
    pl.semaphore_wait(barrier, experts + 1)

    pending = []

    def remote(src, dst, send, recv, peer):
        return pltpu.make_async_remote_copy(
            src_ref=src, dst_ref=dst, send_sem=send, recv_sem=recv,
            device_id=peer, device_id_type=MESH,
        )

    def launch(copy):
        copy.start()
        pending.append(copy)

    own = pltpu.make_async_copy(sent.at[group], rows.at[core, side, group], a_recv.at[group])
    own.start()
    for i, peer in zip(order[1:], peers[1:]):
        launch(remote(
            sent.at[flip(group, i)], rows.at[core, side, group],
            a_send.at[flip(group, i)], a_recv.at[group], peer,
        ))

    logits = lax.dot_general(
        router_ref[...], normed, (((1,), (1,)), ((), ())), preferred_element_type=jnp.float32
    )
    expert_row = lax.broadcasted_iota(jnp.int32, (experts, tok), 0)
    score = [
        jax.nn.sigmoid(
            jnp.sum(jnp.where(expert_row == ids[n : n + 1, :], logits, 0.0), axis=0, keepdims=True)
        )
        for n in range(2)
    ]
    total = score[0] + score[1]
    mix = jnp.where(first, score[0] / total, 0.0) + jnp.where(second, score[1] / total, 0.0)
    mix_high = mix.astype(jnp.bfloat16)
    mix_low = (mix - mix_high.astype(jnp.float32)).astype(jnp.bfloat16)

    def share(which, g):
        launch(remote(
            rows.at[core, which, g], rows.at[core, which, g],
            c_send.at[which, g], c_recv.at[which, g], sibling,
        ))

    def take_neighbour(g):
        remote(
            rows.at[core, other_side, g], rows.at[core, other_side, g],
            x_send.at[g], x_recv.at[g], neighbour,
        ).wait_recv()
        share(other_side, g)

    lag = 3
    places = [flip(group, i) for i in order]
    split = experts // 2

    def step(n):
        g = places[n]
        if n == 0:
            own.wait()
        else:
            remote(
                sent.at[g], rows.at[core, side, g], a_send.at[g], a_recv.at[g], peers[n]
            ).wait_recv()
        launch(remote(
            rows.at[core, side, g], rows.at[core, side, g], x_send.at[g], x_recv.at[g], neighbour
        ))
        share(side, g)
        if n >= lag:
            take_neighbour(places[n - lag])

    for n in range(split + lag):
        step(n)
    tasks = [functools.partial(step, n) for n in range(split + lag, experts)]
    tasks += [functools.partial(take_neighbour, places[n]) for n in range(experts - lag, experts)]

    for load in loads:
        load.wait()

    def feed_forward(part, between):
        members = [(which, places[part * split + n]) for which in (other_side, side) for n in range(split)]
        for which, g in members:
            remote(
                rows.at[other_core, which, g], rows.at[other_core, which, g],
                c_send.at[which, g], c_recv.at[which, g], sibling,
            ).wait_recv()
        hooks = list(between)
        units = hid.shape[1] // tile
        parts = half // tile
        spread = units + 2 * parts
        done = [0]

        def relay():
            done[0] += 1
            while len(hooks) > len(between) * (spread - done[0]) // spread:
                hooks.pop(0)()

        for n in range(units):
            cols = slice(n * tile, (n + 1) * tile)
            low = jnp.concatenate([rows[0, which, g] for which, g in members], axis=0)
            high = jnp.concatenate([rows[1, which, g] for which, g in members], axis=0)

            def project(w):
                return jnp.dot(
                    low, w[:half, cols], preferred_element_type=jnp.float32
                ) + jnp.dot(high, w[half:, cols], preferred_element_type=jnp.float32)

            hid[:, cols] = (jax.nn.silu(project(wg)) * project(wu)).astype(jnp.bfloat16)
            relay()

        def down(which_half, n):
            cols = pl.ds(pl.multiple_of(which_half * half + n * tile, tile), tile)
            return jnp.dot(hid[...], wd[:, cols], preferred_element_type=jnp.float32)

        for n in range(parts):
            cols = slice(n * tile, (n + 1) * tile)
            give[part, :, cols] = down(other_core, n).astype(jnp.bfloat16)
            relay()
        launch(remote(give.at[part], got.at[part], p_send.at[part], p_recv.at[part], sibling))
        for n in range(parts):
            cols = slice(n * tile, (n + 1) * tile)
            acc[part, :, cols] = down(core, n)
            relay()

    def chip_sum(from_side, n):
        part, at = n // split, (from_side * split + n % split) * padded
        at = slice(at, at + padded)
        return acc[part, at, :] + got[part, at, :].astype(jnp.float32)

    def send_across(part):
        remote(give.at[part], got.at[part], p_send.at[part], p_recv.at[part], sibling).wait_recv()
        for n in range(part * split, (part + 1) * split):
            g = places[n]
            cross[g] = chip_sum(0, n).astype(jnp.bfloat16)
            launch(remote(cross.at[g], crossed.at[g], r_send.at[g], r_recv.at[g], neighbour))

    def finish(n):
        g = places[n]
        remote(cross.at[g], crossed.at[g], r_send.at[g], r_recv.at[g], neighbour).wait_recv()
        whole = (chip_sum(1, n) + crossed[g].astype(jnp.float32)).astype(jnp.bfloat16)
        if n == 0:
            back[g] = whole
        else:
            result[g] = whole
            launch(remote(result.at[g], back.at[group], o_send.at[g], o_recv.at[group], peers[n]))

    feed_forward(0, tasks)
    send_across(0)
    feed_forward(1, ())
    send_across(1)
    for n in range(experts):
        finish(n)

    for n, i in enumerate(order[1:], 1):
        g = flip(group, i)
        remote(result.at[g], back.at[g], o_send.at[g], o_recv.at[g], peers[n]).wait_recv()
    returned = back[...].reshape(slots, half)
    combined = sum(
        lax.dot_general(part, returned, (((0,), (0,)), ((), ())), preferred_element_type=jnp.float32)
        for part in (mix_high, mix_low)
    )
    residual = jnp.where(core == 0, states_ref[:, :half], states_ref[:, half:]).astype(jnp.float32)
    final[core] = (residual + combined).astype(jnp.bfloat16)
    last = remote(final.at[core], final.at[core], f_send, f_recv, sibling)
    last.start()
    remote(final.at[other_core], final.at[other_core], f_send, f_recv, sibling).wait_recv()
    out_ref[:, :half] = final[0]
    out_ref[:, half:] = final[1]
    last.wait_send()
    for copy in pending:
        copy.wait_send()


def per_device(states, norm_gain, router, w_gate, w_up, w_down, expert_ids, slot_pos, keep_mask):
    tok, width = states.shape
    groups = lax.axis_size("expert")
    experts = router.shape[1]
    assert groups == 2 * experts and lax.axis_size("tensor") == 2
    capacity = max(2, 5 * tok // (2 * experts) + 1)
    padded = -(-capacity // 16) * 16
    half = width // 2
    slots = experts * padded
    units = w_gate.shape[2]
    bf16, f32 = jnp.bfloat16, jnp.float32
    dma = pltpu.SemaphoreType.DMA
    vmem = pl.BlockSpec(memory_space=pltpu.VMEM)
    hbm = pl.BlockSpec(memory_space=pl.ANY)
    return pl.pallas_call(
        functools.partial(kernel, experts, capacity, padded),
        out_shape=jax.ShapeDtypeStruct((tok, width), bf16),
        in_specs=[vmem] * 6 + [hbm] * 3,
        out_specs=vmem,
        scratch_shapes=[
            pltpu.VMEM((width, units), bf16),
            pltpu.VMEM((width, units), bf16),
            pltpu.VMEM((units, width), bf16),
            pltpu.VMEM((experts, padded, half), bf16),
            pltpu.VMEM((2, 2, experts, padded, half), bf16),
            pltpu.VMEM((slots, units), bf16),
            pltpu.VMEM((2, slots, half), bf16),
            pltpu.VMEM((2, slots, half), bf16),
            pltpu.VMEM((2, slots, half), f32),
            pltpu.VMEM((experts, padded, half), bf16),
            pltpu.VMEM((experts, padded, half), bf16),
            pltpu.VMEM((experts, padded, half), bf16),
            pltpu.VMEM((experts, padded, half), bf16),
            pltpu.VMEM((2, tok, half), bf16),
            dma((3,)),
            dma((experts,)), dma((experts,)),
            dma((2, experts)), dma((2, experts)),
            dma((experts,)), dma((experts,)),
            dma((2,)), dma((2,)),
            dma((experts,)), dma((experts,)),
            dma((experts,)), dma((experts,)),
            dma, dma,
        ],
        compiler_params=pltpu.CompilerParams(
            collective_id=0, has_side_effects=True, vmem_limit_bytes=60 * 1024 * 1024
        ),
    )(states, norm_gain, router.T, expert_ids.T, slot_pos.T, keep_mask.T, w_gate, w_up, w_down)


def solution(mesh):
    placed = (
        P("expert", None),
        P(),
        P(),
        P("expert", None, "tensor"),
        P("expert", None, "tensor"),
        P("expert", "tensor", None),
        P("expert", None),
        P("expert", None),
        P("expert", None),
    )
    return jax.shard_map(
        per_device, mesh=mesh, in_specs=placed, out_specs=P("expert", None), check_vma=False
    )
```
